32 devices in a mesh: groups: 1, row: 4 (over z), col: 4 (over y, x), ksplit: 2 (over core).
Axes of the slice: x: 2, y: 2, z: 4, core: 2. Of those that a mesh axis runs over, the one named last changes fastest.
Arguments:
- pair_state: bfloat16 [128, 128, 128], P(('groups', 'row'), ('col', 'ksplit')), may hold values from -6 to 6
- residue_mask: int32 [128], P('groups'), may hold values 0 or 1
- input_gain: float32 [128], replicated, may hold values from 0.1 to 1.9
- input_shift: float32 [128], replicated, may hold values from -3 to 3
- left_right: bfloat16 [128, 512], replicated, may hold values from -0.5 to 0.5
- output_gate: bfloat16 [128, 128], replicated, may hold values from -0.5 to 0.5
- final_gain: float32 [128], replicated, may hold values from 0.1 to 1.9
- final_shift: float32 [128], replicated, may hold values from -3 to 3
- output_weight: bfloat16 [128, 128], replicated, may hold values from -0.5 to 0.5
Outputs:
- pair_update: bfloat16 [128, 128, 128], P(('groups', 'row'), ('col', 'ksplit'))
The draws below stay inside these ranges and needn't reach their ends.
All inputs are finite; a program needn't handle non-finite values.
Results may differ from the reference program's by a relative error of at most 0.0053.
Values may be sent and summed in bfloat16 or wider, within the bound.
A program may use at most 64 MiB of HBM per device.

```python
import jax
import jax.numpy as jnp
from jax import lax

C = 128
H = 128
N = 128
N_ROW = 4


def plant(entries, rng, smallest, top_value):
    longest = entries.shape.index(max(entries.shape))
    spots = []
    for shift in (0, 1):
        where = [jax.random.randint(jax.random.fold_in(rng, axis), (), 0, length) for axis, length in enumerate(entries.shape)]
        where[longest] = (where[longest] + shift) % entries.shape[longest]
        spots.append(tuple(where))
    return entries.at[spots[0]].set(smallest).at[spots[1]].set(top_value)


def shard_levels(rng, dims, split, smallest, largest):
    level, own = 1.0, jax.random.fold_in(rng, 6)
    for dim, parts in split:
        heights = jnp.exp(jax.random.uniform(jax.random.fold_in(own, dim), (parts,), jnp.float32, smallest / len(split), largest / len(split)))
        level = level * jnp.repeat(heights, dims[dim] // parts).reshape([-1 if axis == dim else 1 for axis in range(len(dims))])
    return level


def scatter_about(own_key, shape, scale, most, pieces=(), held_as=jnp.bfloat16):
    loudness = shard_levels(own_key, shape, pieces, -0.22, 0.18) if pieces else 1.0
    entries = jax.random.normal(own_key, shape, jnp.float32) * scale * loudness
    return jnp.minimum(jnp.maximum(entries, -most), most).astype(held_as)


def setup_inputs(seed: int = 0, part: int = 0) -> dict:
    seeds = jax.random.split(jax.random.key(seed), 10)
    own_keys = jax.random.split(jax.random.fold_in(seeds[9], part), 10)
    return {
        "pair_state": scatter_about(own_keys[0], (N, N, C), 1.0, 6.0, ((0, 4), (1, 8))),
        "residue_mask": plant((jax.random.randint(own_keys[1], (N,), 0, 4) < 3).astype(jnp.int32), jax.random.fold_in(own_keys[1], 1), 0, 1),
        "input_gain": jnp.clip(1.0 + 0.18 * jax.random.normal(seeds[2], (C,), jnp.float32), 0.1, 1.9),
        "input_shift": scatter_about(seeds[3], (C,), 0.5, 3.0, (), jnp.float32),
        "left_right": scatter_about(seeds[4], (C, 4 * H), C ** -0.5, 0.5),
        "output_gate": scatter_about(seeds[5], (C, C), C ** -0.5, 0.5),
        "final_gain": jnp.clip(1.0 + 0.18 * jax.random.normal(seeds[6], (H,), jnp.float32), 0.1, 1.9),
        "final_shift": scatter_about(seeds[7], (H,), 0.5, 3.0, (), jnp.float32),
        "output_weight": scatter_about(seeds[8], (H, C), H ** -0.5, 0.5),
    }


def norm_last(data, norm_gain, norm_shift):
    average = lax.optimization_barrier(jnp.mean(data, axis=-1, keepdims=True))
    centred = data - average
    spread = lax.optimization_barrier(jnp.mean(centred * centred, axis=-1, keepdims=True))
    return centred * lax.rsqrt(spread + 1e-05) * norm_gain + norm_shift

def reference(pair_state, residue_mask, input_gain, input_shift, left_right, output_gate, final_gain, final_shift, output_weight):
    live_rows = residue_mask.astype(jnp.float32)
    block_rows = N // N_ROW
    blocks_state = pair_state.reshape(N_ROW, block_rows, N, C)
    blocks_live = live_rows.reshape(N_ROW, block_rows)

    def one_block(pair):
        state_block, live_block = pair
        normed_block = norm_last(state_block.astype(jnp.float32), input_gain, input_shift).astype(jnp.bfloat16)
        flat_block = normed_block.reshape(block_rows * N, C)
        live_mask = (live_block[:, None] * live_rows[None, :])[:, :, None]
        left_proj = jnp.dot(flat_block, left_right[:, :2 * H], preferred_element_type=jnp.float32).reshape(block_rows, N, 2 * H)
        left_block = (live_mask * jax.nn.sigmoid(left_proj[:, :, H:]) * left_proj[:, :, :H]).astype(jnp.bfloat16)
        right_proj = jnp.dot(flat_block, left_right[:, 2 * H:], preferred_element_type=jnp.float32).reshape(block_rows, N, 2 * H)
        right_block = (live_mask * jax.nn.sigmoid(right_proj[:, :, H:]) * right_proj[:, :, :H]).astype(jnp.bfloat16)
        return (normed_block, left_block, right_block)
    normed_blocks, left_blocks, right_blocks = lax.map(one_block, (blocks_state, blocks_live))
    normed_in = normed_blocks.reshape(N, N, C)
    left_side = left_blocks.reshape(N, N, H)
    right_side = right_blocks.reshape(N, N, H)
    flat_rows = normed_in.reshape(N * N, C)
    left_major = jnp.transpose(left_side, (2, 0, 1))
    right_major = jnp.transpose(right_side, (2, 0, 1))

    def one_channel(pair):
        lhs, rhs = pair
        return jnp.dot(lhs.astype(jnp.float32), rhs.astype(jnp.float32).T, precision=lax.Precision.HIGHEST)
    mixed_all = lax.map(one_channel, (left_major, right_major))
    mixed_last = jnp.transpose(mixed_all, (1, 2, 0))
    normed_out = norm_last(mixed_last, final_gain, final_shift).astype(jnp.bfloat16)
    gate_values = jax.nn.sigmoid(jnp.dot(flat_rows, output_gate, preferred_element_type=jnp.float32))
    projected_out = jnp.dot(normed_out.reshape(N * N, H), output_weight, preferred_element_type=jnp.float32)
    return (gate_values * projected_out).reshape(N, N, C).astype(jnp.bfloat16)
```

```python
import functools

import jax
import jax.numpy as jnp
from jax import lax
from jax.experimental import pallas as pl
from jax.experimental.pallas import tpu as pltpu
from jax.sharding import PartitionSpec as P

MESH = pl.DeviceIdType.MESH
LANES = 128
F32 = jnp.float32
BF16 = jnp.bfloat16
BACK = jnp.bfloat16


def norm_rows(data, gain, shift):
    average = jnp.mean(data, axis=-1, keepdims=True)
    centred = data - average
    spread = jnp.mean(centred * centred, axis=-1, keepdims=True)
    return centred * lax.rsqrt(spread + 1e-05) * gain + shift


def swap_blocks(parts, width):
    count = len(parts)
    lane_block = lax.broadcasted_iota(jnp.int32, parts[0].shape, 1) // width
    parts = list(parts)
    step = count // 2
    while step:
        upper = (lane_block & step) != 0
        for low in range(count):
            if low & step:
                continue
            first, second = parts[low], parts[low + step]
            parts[low] = jnp.where(upper, pltpu.roll(second, step * width, 1), first)
            parts[low + step] = jnp.where(
                upper, second, pltpu.roll(first, LANES - step * width, 1)
            )
        step //= 2
    return parts


def kernel(sizes, *refs):
    row_count, col_count, split_count, tile_rows, tile_cols, channels, hidden = sizes
    hbm_inputs, out_ref, inputs = refs[:9], refs[9], refs[10:19]
    normed_buf, gate_buf, left_stage, right_stage = refs[19:23]
    left_send, right_send, left_recv, right_recv, pieces = refs[23:28]
    load_sem, sent_sem, left_in, right_in, back_in, cross_sem, far_sem = refs[28:35]
    state_ref, mask_ref, input_gain, input_shift, left_right = inputs[:5]
    output_gate, final_gain, final_shift, output_weight = inputs[5:]
    plane = col_count * split_count
    owners = plane * row_count // 2
    half_rows = row_count // 2
    blocks = LANES // tile_rows
    home, back = pieces.at[pl.ds(0, owners)], pieces.at[pl.ds(owners, owners)]
    my_row = lax.axis_index("row")
    my_plane = lax.axis_index("col") * split_count + lax.axis_index("ksplit")
    my_half = my_row // half_rows
    my_inner = lax.rem(my_row, half_rows)
    my_group = my_inner * plane + my_plane
    first_row = my_half * half_rows
    near_row = first_row + 1 - my_inner
    far_close = half_rows - my_half
    far_last = (row_count - 1) * (1 - my_half)

    def place(row, position):
        return {
            "row": row,
            "col": position // split_count,
            "ksplit": lax.rem(position, split_count),
        }

    def peer(step):
        return lax.rem(my_plane + step, plane)

    loads = [
        pltpu.make_async_copy(source, target, load_sem.at[at])
        for at, (source, target) in enumerate(zip(hbm_inputs, inputs))
    ]
    for at in (0, 2, 3, 4, 1, 5, 8, 6, 7):
        loads[at].start()

    barrier = pltpu.get_barrier_semaphore()

    def greet(row, position):
        pl.semaphore_signal(
            barrier, inc=1, device_id=place(row, position), device_id_type=MESH
        )

    for step in range(1, plane):
        greet(my_row, peer(step))
    greet(near_row, my_plane)

    @pl.when(my_half == 0)
    def _():
        for row in range(half_rows, row_count):
            for step in range(plane):
                greet(row, peer(step))

    def tell(sem, row):
        pl.semaphore_signal(
            sem, inc=1, device_id=place(row, my_plane), device_id_type=MESH
        )

    for at in (0, 2, 3):
        loads[at].wait()

    positions = tile_rows * tile_cols
    state = state_ref[...].astype(F32).reshape(positions, channels)
    normed = norm_rows(state, input_gain[...], input_shift[...]).astype(BF16)
    normed_buf[...] = normed.astype(F32)
    loads[4].wait()
    loads[1].wait()
    weights = jnp.transpose(left_right[...].astype(F32)).astype(BF16)

    lane = lax.broadcasted_iota(jnp.int32, (1, LANES), 1)
    lane_block = lax.broadcasted_iota(jnp.int32, (tile_rows, LANES), 1) // tile_rows
    mask_line = mask_ref[...].astype(F32)
    mask_rows = jnp.broadcast_to(mask_line, (tile_rows, LANES))
    row_live = mask_rows
    turn = lax.rem(lane_block - my_row + row_count, row_count)
    for shift in range(1, blocks):
        row_live = jnp.where(turn == shift, pltpu.roll(mask_rows, shift * tile_rows, 1), row_live)

    lives, packs = [], []
    for quarter in range(tile_cols // blocks):
        rows = []
        col_live = jnp.zeros((tile_rows, LANES), F32)
        for inner in range(blocks):
            k = quarter * blocks + inner
            rows.append(normed_buf[pl.ds(k, tile_rows, stride=tile_cols), :])
            alive = jnp.where(lane == my_plane * tile_cols + k, mask_line, 0.0)
            alive = jnp.sum(alive, axis=1, keepdims=True)
            col_live = jnp.where(lane_block == inner, alive, col_live)
        lives.append(row_live * col_live)
        packs.append(jnp.concatenate(rows, axis=0).astype(BF16))

    def make_side(side, stage, ready):
        own = weights[side * 2 * hidden : (side + 1) * 2 * hidden]
        for quarter in range(tile_cols // blocks):
            projected = lax.dot_general(
                own, packs[quarter], (((1,), (1,)), ((), ())), preferred_element_type=F32
            )
            parts = []
            for block in range(blocks):
                at = block * tile_rows
                value = projected[at : at + tile_rows]
                gate = projected[at + hidden : at + hidden + tile_rows]
                parts.append(lives[quarter] * jax.nn.sigmoid(gate) * value)
            swapped = swap_blocks(parts, tile_rows)
            for inner in range(blocks):
                k = quarter * blocks + inner
                stage[pl.ds(k, tile_rows, stride=tile_cols), :] = swapped[inner]
        ready[...] = stage[...].reshape(ready.shape).astype(BF16)

    def send_right(row, position):
        group = lax.rem(row, half_rows) * plane + position
        pltpu.make_async_remote_copy(
            src_ref=right_send.at[:, group],
            dst_ref=right_recv.at[:, my_row, my_plane],
            send_sem=sent_sem.at[0],
            recv_sem=right_in.at[my_row],
            device_id=place(row, position),
            device_id_type=MESH,
        ).start()

    def send_left(row, position):
        group = lax.rem(row, half_rows) * plane + position
        pltpu.make_async_remote_copy(
            src_ref=left_send.at[:, group],
            dst_ref=left_recv.at[:, my_inner, my_plane],
            send_sem=sent_sem.at[1],
            recv_sem=left_in.at[my_inner],
            device_id=place(row, position),
            device_id_type=MESH,
        ).start()

    def send_back(inner, position, group):
        pltpu.make_async_remote_copy(
            src_ref=back.at[group],
            dst_ref=home.at[my_group],
            send_sem=sent_sem.at[2],
            recv_sem=back_in.at[0],
            device_id=place(first_row + inner, position),
            device_id_type=MESH,
        ).start()

    def wait_bytes(ref, sem):
        pltpu.make_async_copy(ref, ref, sem).wait()

    make_side(1, right_stage, right_send)
    pl.semaphore_wait(barrier, plane + my_half * owners)
    tell(cross_sem.at[0], near_row)

    @pl.when(my_half == 1)
    def _():
        for row in range(half_rows):
            tell(far_sem.at[my_inner], row)
        for row in (1, 0):
            for step in range(plane):
                send_right(row, peer(step))

    for step in range(1, plane):
        send_right(my_row, peer(step))
    right_recv[:, my_row, my_plane] = right_send[:, my_group]
    make_side(0, left_stage, left_send)
    for step in range(1, plane):
        send_left(my_row, peer(step))
    pl.semaphore_wait(cross_sem.at[0], 1)
    for step in range(plane):
        send_left(near_row, peer(step))
    for step in range(plane):
        send_right(near_row, peer(step))

    left_recv[:, my_inner, my_plane] = left_send[:, my_group]
    for at in (5, 8, 6, 7):
        loads[at].wait()
    gates = jnp.dot(normed, output_gate[...], preferred_element_type=F32)
    gate_buf[...] = jax.nn.sigmoid(gates)

    @pl.when(my_half == 0)
    def _():
        for inner in range(half_rows):
            pl.semaphore_wait(far_sem.at[inner], 1)
            for step in range(plane):
                send_right(half_rows + inner, peer(step))

    wait_bytes(left_recv.at[:, my_inner, pl.ds(0, plane - 1)], left_in.at[my_inner])
    wait_bytes(left_recv.at[:, 1 - my_inner], left_in.at[1 - my_inner])

    depth = plane * tile_cols
    half_bit = (lax.broadcasted_iota(jnp.int32, (tile_rows, LANES), 1) // tile_cols) & 1
    lefts = []
    for bit in range(2):
        both = [
            jnp.transpose(left_recv[bit, inner].reshape(depth, LANES).astype(F32))
            for inner in range(half_rows)
        ]
        lefts.append(jnp.concatenate(both, axis=0).astype(BF16))

    for row in (my_row, near_row, far_close, far_last):
        if row is my_row:
            wait_bytes(right_recv.at[:, row, pl.ds(0, plane - 1)], right_in.at[row])
        else:
            wait_bytes(right_recv.at[:, row], right_in.at[row])
        products = [
            jnp.dot(
                lefts[bit], right_recv[bit, row].reshape(depth, LANES), preferred_element_type=F32
            )
            for bit in range(2)
        ]
        for inner in range(half_rows):
            mixed = []
            for product in products:
                piece = product[inner * LANES : (inner + 1) * LANES]
                chosen = piece[:tile_rows]
                for block in range(1, blocks):
                    chosen = jnp.where(
                        lane_block == block,
                        piece[block * tile_rows : (block + 1) * tile_rows],
                        chosen,
                    )
                mixed.append(chosen)
            first = jnp.where(half_bit == 0, mixed[0], pltpu.roll(mixed[1], tile_cols, 1))
            second = jnp.where(
                half_bit == 1, mixed[1], pltpu.roll(mixed[0], LANES - tile_cols, 1)
            )
            for half, part in ((0, first), (1, second)):
                position = row * 2 + half
                group = inner * plane + position
                back[group] = part.astype(BACK)

                @pl.when(group != my_group)
                def _():
                    send_back(inner, position, group)

                @pl.when(group == my_group)
                def _():
                    home[my_group] = back[my_group]

    wait_bytes(home.at[pl.ds(0, owners - 1)], back_in.at[0])

    left_stage[...] = home[...].astype(F32).reshape(owners * tile_rows, LANES)
    step_rows = LANES // tile_cols
    for group in range(tile_rows // step_rows):
        rows = [
            left_stage[pl.ds(group * step_rows + at, owners, stride=tile_rows), :]
            for at in range(step_rows)
        ]
        turned = jnp.transpose(jnp.concatenate(rows, axis=0))
        parts = [turned[b * tile_cols : (b + 1) * tile_cols] for b in range(step_rows)]
        together = jnp.concatenate(swap_blocks(parts, owners), axis=0)
        normed_out = norm_rows(together, final_gain[...], final_shift[...]).astype(BF16)
        projected_out = jnp.dot(normed_out, output_weight[...], preferred_element_type=F32)
        gated = gate_buf[group * LANES : (group + 1) * LANES] * projected_out
        out_ref[group * step_rows : (group + 1) * step_rows] = gated.reshape(
            step_rows, tile_cols, channels
        ).astype(BF16)

    wait_bytes(pieces.at[pl.ds(0, 2 * owners - 1)], sent_sem.at[0])
    wait_bytes(pieces.at[pl.ds(0, owners - 1)], sent_sem.at[1])
    wait_bytes(pieces.at[pl.ds(0, owners - 1)], sent_sem.at[2])


def fused(sizes, *arrays):
    row_count, col_count, split_count, tile_rows, tile_cols, channels, hidden = sizes
    plane = col_count * split_count
    owners = row_count * plane // 2
    state, *lines, weights, gate, gain_out, shift_out, weight_out = arrays
    lines = [line[None] for line in lines]
    operands = [state, *lines, weights, gate, gain_out[None], shift_out[None], weight_out]
    flat = (tile_rows * tile_cols, LANES)
    tile = (tile_cols, LANES)
    counts = (len(operands), 3, row_count // 2, row_count, 1)
    return pl.pallas_call(
        functools.partial(kernel, sizes),
        out_shape=pltpu.VMEM(state.shape, BF16),
        in_specs=[pl.BlockSpec(memory_space=pl.ANY)] * len(operands),
        out_specs=pl.BlockSpec(memory_space=pltpu.VMEM),
        scratch_shapes=[pltpu.VMEM(item.shape, item.dtype) for item in operands]
        + [pltpu.VMEM(flat, F32)] * 4
        + [pltpu.VMEM((2, owners) + tile, BF16)] * 2
        + [
            pltpu.VMEM((2, row_count // 2, plane) + tile, BF16),
            pltpu.VMEM((2, row_count, plane) + tile, BF16),
            pltpu.VMEM((2 * owners, tile_rows, LANES), BACK),
        ]
        + [pltpu.SemaphoreType.DMA((count,)) for count in counts]
        + [pltpu.SemaphoreType.REGULAR((count,)) for count in (1, 2)],
        compiler_params=pltpu.CompilerParams(collective_id=0, has_side_effects=True),
    )(*operands)


def update(*arrays):
    state, mask, weight_out = arrays[0], arrays[1], arrays[8]
    tile_rows, tile_cols, channels = state.shape
    hidden = weight_out.shape[0]
    row_count, col_count = lax.axis_size("row"), lax.axis_size("col")
    split_count = lax.axis_size("ksplit")
    devices = row_count * col_count * split_count
    fits = (
        channels == LANES
        and hidden == LANES
        and mask.shape[0] == LANES
        and row_count * tile_rows == LANES
        and devices == tile_rows
        and row_count == 4
        and devices // 2 == tile_cols
        and tile_rows == 2 * tile_cols
        and tile_cols % 16 == 0
    )
    if fits:
        sizes = (row_count, col_count, split_count, tile_rows, tile_cols, channels, hidden)
        return fused(sizes, *arrays)
    return body(*arrays)


def norm_over(data, norm_gain, norm_shift, over_axis):
    average = jnp.mean(data, axis=over_axis, keepdims=True)
    centred = data - average
    spread = jnp.mean(centred * centred, axis=over_axis, keepdims=True)
    return centred * lax.rsqrt(spread + 1e-05) * norm_gain + norm_shift


def gated_side(normed_in, weights, live_mask, hidden):
    values = jnp.einsum(
        "ikc,ch->hik", normed_in, weights[:, :hidden], preferred_element_type=jnp.float32
    )
    gates = jnp.einsum(
        "ikc,ch->hik", normed_in, weights[:, hidden:], preferred_element_type=jnp.float32
    )
    return (live_mask * jax.nn.sigmoid(gates) * values).astype(jnp.bfloat16)


def contract_parts(left_parts, right_parts, row_count, col_count):
    count_items = left_parts.shape[2]
    tile_rows = left_parts.shape[3]
    tile_cols = left_parts.shape[4]

    def assemble(parts):
        return parts.transpose(2, 0, 3, 1, 4).reshape(
            count_items, row_count * tile_rows, col_count * tile_cols
        )

    products = jnp.einsum(
        "cik,cjk->cij",
        assemble(left_parts),
        assemble(right_parts),
        preferred_element_type=jnp.float32,
    )
    returned = products.reshape(count_items, row_count, tile_rows, col_count, tile_cols)
    return returned.transpose(1, 3, 0, 2, 4)


def body(
    pair_state,
    residue_mask,
    input_gain,
    input_shift,
    left_right,
    output_gate,
    final_gain,
    final_shift,
    output_weight,
):
    tile_rows, tile_cols, channels = pair_state.shape
    hidden = output_weight.shape[0]
    normed_in = norm_over(pair_state.astype(jnp.float32), input_gain, input_shift, 2).astype(
        jnp.bfloat16
    )
    row_start = lax.axis_index("row") * tile_rows
    col_start = lax.axis_index(("col", "ksplit")) * tile_cols
    row_live = lax.dynamic_slice_in_dim(residue_mask, row_start, tile_rows).astype(jnp.float32)
    col_live = lax.dynamic_slice_in_dim(residue_mask, col_start, tile_cols).astype(jnp.float32)
    live_mask = row_live[:, None] * col_live[None, :]
    left_side = gated_side(normed_in, left_right[:, : 2 * hidden], live_mask, hidden)
    right_side = gated_side(normed_in, left_right[:, 2 * hidden :], live_mask, hidden)
    devices_all = lax.axis_size(("row", "col", "ksplit"))
    row_count = lax.axis_size("row")
    col_count = devices_all // row_count
    per_device = hidden // devices_all
    grouped_left = left_side.reshape(devices_all, per_device, tile_rows, tile_cols)
    grouped_right = right_side.reshape(devices_all, per_device, tile_rows, tile_cols)
    left_parts = lax.all_to_all(
        grouped_left, ("row", "col", "ksplit"), split_axis=0, concat_axis=0, tiled=True
    )
    right_parts = lax.all_to_all(
        grouped_right, ("row", "col", "ksplit"), split_axis=0, concat_axis=0, tiled=True
    )
    count_items = left_parts.shape[1]
    shaped_left = left_parts.reshape(row_count, col_count, count_items, tile_rows, tile_cols)
    shaped_right = right_parts.reshape(row_count, col_count, count_items, tile_rows, tile_cols)
    returned = contract_parts(shaped_left, shaped_right, row_count, col_count)
    returned = returned.reshape(devices_all, count_items, tile_rows, tile_cols)
    received = lax.all_to_all(
        returned, ("row", "col", "ksplit"), split_axis=0, concat_axis=0, tiled=True
    )
    mixed_tile = received.reshape(hidden, tile_rows, tile_cols)
    normed_out = norm_over(
        mixed_tile, final_gain[:, None, None], final_shift[:, None, None], 0
    ).astype(jnp.bfloat16)
    projected_out = jnp.einsum(
        "hij,hc->ijc", normed_out, output_weight, preferred_element_type=jnp.float32
    )
    gate_values = jax.nn.sigmoid(
        jnp.einsum("ijc,cd->ijd", normed_in, output_gate, preferred_element_type=jnp.float32)
    )
    return (gate_values * projected_out).astype(jnp.bfloat16)


def solution(mesh):
    placed = (
        P(("groups", "row"), ("col", "ksplit"), None),
        P("groups"),
        P(),
        P(),
        P(),
        P(),
        P(),
        P(),
        P(),
    )
    return jax.shard_map(
        update,
        mesh=mesh,
        in_specs=placed,
        out_specs=P(("groups", "row"), ("col", "ksplit"), None),
        check_vma=False,
    )
```

```python
import functools

import jax
import jax.numpy as jnp
from jax import lax
from jax.experimental import pallas as pl
from jax.experimental.pallas import tpu as pltpu
from jax.sharding import PartitionSpec as P

MESH = pl.DeviceIdType.MESH
LANES = 128
F32 = jnp.float32
BF16 = jnp.bfloat16
BACK = jnp.bfloat16


def norm_rows(data, gain, shift):
    average = jnp.mean(data, axis=-1, keepdims=True)
    centred = data - average
    spread = jnp.mean(centred * centred, axis=-1, keepdims=True)
    return centred * lax.rsqrt(spread + 1e-05) * gain + shift


def swap_blocks(parts, width):
    count = len(parts)
    lane_block = lax.broadcasted_iota(jnp.int32, parts[0].shape, 1) // width
    parts = list(parts)
    step = count // 2
    while step:
        upper = (lane_block & step) != 0
        for low in range(count):
            if low & step:
                continue
            first, second = parts[low], parts[low + step]
            parts[low] = jnp.where(upper, pltpu.roll(second, step * width, 1), first)
            parts[low + step] = jnp.where(
                upper, second, pltpu.roll(first, LANES - step * width, 1)
            )
        step //= 2
    return parts


def kernel(sizes, *refs):
    row_count, col_count, split_count, tile_rows, tile_cols, channels, hidden = sizes
    (state_hbm, mask_hbm, input_gain_hbm, input_shift_hbm, left_right_hbm) = refs[:5]
    (output_gate_hbm, final_gain_hbm, final_shift_hbm, output_weight_hbm) = refs[5:9]
    out_ref, state_ref, mask_ref, lines, left_right, squares = refs[9:15]
    normed_buf, normed_wide, gate_buf, left_stage, right_stage, home_stage = refs[15:21]
    left_send, right_send, left_recv, right_recv, pieces = refs[21:26]
    load_sem, sent_sem, left_in, right_in, back_in, ready_sem = refs[26:32]
    plane = col_count * split_count
    half_rows = row_count // 2
    owners = plane * half_rows
    blocks = LANES // tile_rows
    quarters = tile_cols // blocks
    home, back = pieces.at[pl.ds(0, owners)], pieces.at[pl.ds(owners, owners)]
    my_row = lax.axis_index("row")
    my_plane = lax.axis_index("col") * split_count + lax.axis_index("ksplit")
    my_col, my_split = lax.axis_index("col"), lax.axis_index("ksplit")
    my_half = my_row // half_rows
    my_inner = lax.rem(my_row, half_rows)
    my_group = my_inner * plane + my_plane
    first_row = my_half * half_rows
    near_row = first_row + 1 - my_inner

    def place(row, position):
        return {
            "row": row,
            "col": position // split_count,
            "ksplit": lax.rem(position, split_count),
        }

    def peer(step):
        return lax.rem(my_plane + step, plane)

    def load(source, target, at):
        pltpu.make_async_copy(source, target, load_sem.at[at]).start()

    def wait_bytes(ref, sem):
        pltpu.make_async_copy(ref, ref, sem).wait()

    wide = 2 * hidden
    for at in range(quarters):
        part = pl.ds(at * (tile_rows // quarters), tile_rows // quarters)
        load(state_hbm.at[part], state_ref.at[part], 0)
    load(mask_hbm, mask_ref, 1)
    load(input_gain_hbm, lines.at[0], 2)
    load(input_shift_hbm, lines.at[1], 2)
    load(final_gain_hbm, lines.at[2], 2)
    load(final_shift_hbm, lines.at[3], 2)
    load(left_right_hbm.at[:, pl.ds(wide, wide)], left_right.at[1], 4)
    load(left_right_hbm.at[:, pl.ds(0, wide)], left_right.at[0], 3)
    load(output_gate_hbm, squares.at[0], 5)
    load(output_weight_hbm, squares.at[1], 5)

    barrier = pltpu.get_barrier_semaphore()

    def greet(row, position):
        pl.semaphore_signal(
            barrier, inc=1, device_id=place(row, position), device_id_type=MESH
        )

    for step in range(1, plane):
        greet(my_row, peer(step))
    for row in range(1, row_count):

        @pl.when(my_row < row)
        def _():
            for step in range(plane):
                greet(row, peer(step))

    def announce():
        pl.semaphore_wait(barrier, plane - 1 + my_row * plane)
        for row in range(row_count - 1):

            hears = (my_row > row) & (my_row <= row + half_rows)

            @pl.when(hears & (my_split == split_count - 1))
            def _():
                for split in range(split_count):
                    pl.semaphore_signal(
                        ready_sem.at[my_row - 1],
                        inc=1,
                        device_id={"row": row, "col": my_col, "ksplit": split},
                        device_id_type=MESH,
                    )

    wait_bytes(mask_ref, load_sem.at[1])
    lane = lax.broadcasted_iota(jnp.int32, (1, LANES), 1)
    lane_block = lax.broadcasted_iota(jnp.int32, (tile_rows, LANES), 1) // tile_rows
    mask_line = mask_ref[...].astype(F32)
    mask_rows = jnp.broadcast_to(mask_line, (tile_rows, LANES))
    row_live = mask_rows
    turn = lax.rem(lane_block - my_row + row_count, row_count)
    for shift in range(1, blocks):
        row_live = jnp.where(turn == shift, pltpu.roll(mask_rows, shift * tile_rows, 1), row_live)
    lives = []
    for quarter in range(quarters):
        col_live = jnp.zeros((tile_rows, LANES), F32)
        for inner in range(blocks):
            k = quarter * blocks + inner
            alive = jnp.where(lane == my_plane * tile_cols + k, mask_line, 0.0)
            alive = jnp.sum(alive, axis=1, keepdims=True)
            col_live = jnp.where(lane_block == inner, alive, col_live)
        lives.append(row_live * col_live)

    wait_bytes(lines, load_sem.at[2])
    wait_bytes(state_ref, load_sem.at[0])
    positions = tile_rows * tile_cols
    state = state_ref[...].astype(F32).reshape(positions, channels)
    normed = norm_rows(state, lines[0], lines[1])
    normed_wide[...] = normed.astype(BF16)
    for at in range(tile_rows):
        normed_buf[pl.ds(at * (tile_cols + 1), tile_cols), :] = normed[
            at * tile_cols : (at + 1) * tile_cols
        ]
    packs = []
    for quarter in range(quarters):
        rows = [
            normed_buf[pl.ds(quarter * blocks + inner, tile_rows, stride=tile_cols + 1), :]
            for inner in range(blocks)
        ]
        packs.append(jnp.concatenate(rows, axis=0).astype(BF16))

    def make_side(side, stage, ready):
        wait_bytes(left_right.at[side], load_sem.at[3 + side])
        own = jnp.transpose(left_right[side].astype(F32)).astype(BF16)
        for quarter in range(quarters):
            projected = lax.dot_general(
                own, packs[quarter], (((1,), (1,)), ((), ())), preferred_element_type=F32
            )
            parts = []
            for block in range(blocks):
                at = block * tile_rows
                value = projected[at : at + tile_rows]
                gate = projected[at + hidden : at + hidden + tile_rows]
                parts.append(lives[quarter] * jax.nn.sigmoid(gate) * value)
            swapped = swap_blocks(parts, tile_rows)
            for inner in range(blocks):
                k = quarter * blocks + inner
                stage[pl.ds(k, tile_rows, stride=tile_cols + 1), :] = swapped[inner]
        for at in range(tile_rows):
            ready[at // owners, at % owners] = stage[
                pl.ds(at * (tile_cols + 1), tile_cols), :
            ].astype(BF16)

    def send_right(row, position):
        group = lax.rem(row, half_rows) * plane + position
        pltpu.make_async_remote_copy(
            src_ref=right_send.at[:, group],
            dst_ref=right_recv.at[:, my_row, my_plane],
            send_sem=sent_sem.at[0],
            recv_sem=right_in.at[my_row],
            device_id=place(row, position),
            device_id_type=MESH,
        ).start()

    def send_left(row, position):
        group = lax.rem(row, half_rows) * plane + position
        pltpu.make_async_remote_copy(
            src_ref=left_send.at[:, group],
            dst_ref=left_recv.at[:, my_inner, my_plane],
            send_sem=sent_sem.at[1],
            recv_sem=left_in.at[0],
            device_id=place(row, position),
            device_id_type=MESH,
        ).start()

    def send_back(inner, position, group):
        pltpu.make_async_remote_copy(
            src_ref=back.at[group],
            dst_ref=home.at[my_group],
            send_sem=sent_sem.at[2],
            recv_sem=back_in.at[0],
            device_id=place(first_row + inner, position),
            device_id_type=MESH,
        ).start()

    @pl.when(my_col == col_count - 1)
    def _():
        announce()

    make_side(1, right_stage, right_send)
    @pl.when(my_col < col_count - 1)
    def _():
        announce()

    pltpu.make_async_copy(
        right_send.at[:, my_group], right_recv.at[:, my_row, my_plane], right_in.at[my_row]
    ).start()

    known = {row: set(range(row + 1)) for row in range(row_count)}

    def send_all(own_row, plan):
        for send, row in plan:
            if row is None:
                pl.semaphore_wait(ready_sem.at[half_rows - 1], 1)
                continue
            if row not in known[own_row]:
                known[own_row].add(row)
                pl.semaphore_wait(ready_sem.at[row - 1], 1)
            for step in range(1 if row == own_row else 0, plane):
                send(row, peer(step))

    right, left = send_right, send_left
    before = {
        0: (),
        1: (),
        2: (),
        3: (),
    }
    after = {
        0: ((right, 0), (left, 0), (right, 1), (left, 1), (None, None),),
        1: ((left, 0), (right, 0), (left, 1), (right, 1), (right, 2), (right, 3),),
        2: ((right, 0), (left, 3), (right, 1), (left, 2), (right, 3), (right, 2),),
        3: ((left, 2), (right, 0), (right, 1), (left, 3), (right, 2), (right, 3),),
    }

    for row in range(row_count):

        @pl.when(my_row == row)
        def _():
            send_all(row, before[row])

    make_side(0, left_stage, left_send)
    pltpu.make_async_copy(
        left_send.at[:, my_group], left_recv.at[:, my_inner, my_plane], left_in.at[0]
    ).start()
    for row in range(row_count):

        @pl.when(my_row == row)
        def _():
            send_all(row, after[row])

    wait_bytes(squares, load_sem.at[5])
    gates = jnp.dot(normed_wide[...], squares[0], preferred_element_type=F32)
    gate_buf[...] = jax.nn.sigmoid(gates)

    @pl.when(my_half == 0)
    def _():
        wait_bytes(right_recv.at[:, 0], right_in.at[0])
        pltpu.make_async_remote_copy(
            src_ref=right_recv.at[:, 0],
            dst_ref=right_recv.at[:, 0],
            send_sem=sent_sem.at[3],
            recv_sem=right_in.at[0],
            device_id={"row": my_row + half_rows},
            device_id_type=MESH,
        ).start()

    wait_bytes(left_recv, left_in.at[0])

    depth = plane * tile_cols
    half_bit = (lax.broadcasted_iota(jnp.int32, (tile_rows, LANES), 1) // tile_cols) & 1
    lefts = []
    for bit in range(2):
        both = [
            jnp.transpose(left_recv[bit, inner].reshape(depth, LANES).astype(F32))
            for inner in range(half_rows)
        ]
        lefts.append(jnp.concatenate(both, axis=0).astype(BF16))

    for row in range(row_count):
        if row:
            wait_bytes(right_recv.at[:, row], right_in.at[row])
        else:

            @pl.when(my_half == 1)
            def _():
                wait_bytes(right_recv.at[:, 0], right_in.at[0])

        products = [
            jnp.dot(
                lefts[bit], right_recv[bit, row].reshape(depth, LANES), preferred_element_type=F32
            )
            for bit in range(2)
        ]
        for inner in range(half_rows):
            mixed = []
            for product in products:
                piece = product[inner * LANES : (inner + 1) * LANES]
                chosen = piece[:tile_rows]
                for block in range(1, blocks):
                    chosen = jnp.where(
                        lane_block == block,
                        piece[block * tile_rows : (block + 1) * tile_rows],
                        chosen,
                    )
                mixed.append(chosen)
            first = jnp.where(half_bit == 0, mixed[0], pltpu.roll(mixed[1], tile_cols, 1))
            second = jnp.where(
                half_bit == 1, mixed[1], pltpu.roll(mixed[0], LANES - tile_cols, 1)
            )
            for core, part in ((0, first), (1, second)):
                position = row * 2 + core
                group = inner * plane + position
                back[group] = part.astype(BACK)

                @pl.when(group != my_group)
                def _():
                    send_back(inner, position, group)

                @pl.when(group == my_group)
                def _():
                    pltpu.make_async_copy(
                        back.at[group], home.at[my_group], back_in.at[0]
                    ).start()

    wait_bytes(home, back_in.at[0])

    for at in range(owners):
        home_stage[pl.ds(at * (tile_rows + 1), tile_rows), :] = home[at].astype(F32)
    step_rows = LANES // tile_cols
    for group in range(tile_rows // step_rows):
        rows = [
            home_stage[pl.ds(group * step_rows + at, owners, stride=tile_rows + 1), :]
            for at in range(step_rows)
        ]
        turned = jnp.transpose(jnp.concatenate(rows, axis=0))
        parts = [turned[b * tile_cols : (b + 1) * tile_cols] for b in range(step_rows)]
        together = jnp.concatenate(swap_blocks(parts, owners), axis=0)
        normed_out = norm_rows(together, lines[2], lines[3]).astype(BF16)
        projected_out = jnp.dot(normed_out, squares[1], preferred_element_type=F32)
        gated = gate_buf[group * LANES : (group + 1) * LANES] * projected_out
        out_ref[group * step_rows : (group + 1) * step_rows] = gated.reshape(
            step_rows, tile_cols, channels
        ).astype(BF16)

    @pl.when(my_row == 0)
    def _():
        wait_bytes(pieces.at[pl.ds(0, owners - 1)], sent_sem.at[0])

    @pl.when(my_row > 0)
    def _():
        wait_bytes(pieces.at[pl.ds(0, 2 * owners - 1)], sent_sem.at[0])

    @pl.when(my_half == 0)
    def _():
        wait_bytes(right_recv.at[:, 0], sent_sem.at[3])

    wait_bytes(pieces.at[pl.ds(0, owners - 1)], sent_sem.at[1])
    wait_bytes(pieces.at[pl.ds(0, owners - 1)], sent_sem.at[2])


def fused(sizes, *arrays):
    row_count, col_count, split_count, tile_rows, tile_cols, channels, hidden = sizes
    plane = col_count * split_count
    owners = row_count * plane // 2
    state, *lines, weights, gate, gain_out, shift_out, weight_out = arrays
    lines = [line[None] for line in lines]
    operands = [state, *lines, weights, gate, gain_out[None], shift_out[None], weight_out]
    flat = (tile_rows * tile_cols, LANES)
    padded = (tile_rows * (tile_cols + 1), LANES)
    tile = (tile_cols, LANES)
    return pl.pallas_call(
        functools.partial(kernel, sizes),
        out_shape=pltpu.VMEM(state.shape, BF16),
        in_specs=[pl.BlockSpec(memory_space=pl.ANY)] * len(operands),
        out_specs=pl.BlockSpec(memory_space=pltpu.VMEM),
        scratch_shapes=[
            pltpu.VMEM(state.shape, BF16),
            pltpu.VMEM((1, LANES), jnp.int32),
            pltpu.VMEM((4, 1, LANES), F32),
            pltpu.VMEM((2, channels, 2 * hidden), BF16),
            pltpu.VMEM((2, channels, hidden), BF16),
            pltpu.VMEM(padded, F32),
            pltpu.VMEM(flat, BF16),
            pltpu.VMEM(flat, F32),
            pltpu.VMEM(padded, F32),
            pltpu.VMEM(padded, F32),
            pltpu.VMEM((owners * (tile_rows + 1), LANES), F32),
            pltpu.VMEM((2, owners) + tile, BF16),
            pltpu.VMEM((2, owners) + tile, BF16),
            pltpu.VMEM((2, row_count // 2, plane) + tile, BF16),
            pltpu.VMEM((2, row_count, plane) + tile, BF16),
            pltpu.VMEM((2 * owners, tile_rows, LANES), BACK),
        ]
        + [pltpu.SemaphoreType.DMA((count,)) for count in (6, 4, 1, row_count, 1)]
        + [pltpu.SemaphoreType.REGULAR((count,)) for count in (row_count - 1,)],
        compiler_params=pltpu.CompilerParams(collective_id=0, has_side_effects=True),
    )(*operands)


def update(*arrays):
    state, mask, weight_out = arrays[0], arrays[1], arrays[8]
    tile_rows, tile_cols, channels = state.shape
    hidden = weight_out.shape[0]
    row_count, col_count = lax.axis_size("row"), lax.axis_size("col")
    split_count = lax.axis_size("ksplit")
    devices = row_count * col_count * split_count
    fits = (
        channels == LANES
        and hidden == LANES
        and mask.shape[0] == LANES
        and row_count * tile_rows == LANES
        and devices == tile_rows
        and row_count == 4
        and devices // 2 == tile_cols
        and tile_rows == 2 * tile_cols
        and tile_cols % 16 == 0
    )
    if fits:
        sizes = (row_count, col_count, split_count, tile_rows, tile_cols, channels, hidden)
        return fused(sizes, *arrays)
    return body(*arrays)


def norm_over(data, norm_gain, norm_shift, over_axis):
    average = jnp.mean(data, axis=over_axis, keepdims=True)
    centred = data - average
    spread = jnp.mean(centred * centred, axis=over_axis, keepdims=True)
    return centred * lax.rsqrt(spread + 1e-05) * norm_gain + norm_shift


def gated_side(normed_in, weights, live_mask, hidden):
    values = jnp.einsum(
        "ikc,ch->hik", normed_in, weights[:, :hidden], preferred_element_type=jnp.float32
    )
    gates = jnp.einsum(
        "ikc,ch->hik", normed_in, weights[:, hidden:], preferred_element_type=jnp.float32
    )
    return (live_mask * jax.nn.sigmoid(gates) * values).astype(jnp.bfloat16)


def contract_parts(left_parts, right_parts, row_count, col_count):
    count_items = left_parts.shape[2]
    tile_rows = left_parts.shape[3]
    tile_cols = left_parts.shape[4]

    def assemble(parts):
        return parts.transpose(2, 0, 3, 1, 4).reshape(
            count_items, row_count * tile_rows, col_count * tile_cols
        )

    products = jnp.einsum(
        "cik,cjk->cij",
        assemble(left_parts),
        assemble(right_parts),
        preferred_element_type=jnp.float32,
    )
    returned = products.reshape(count_items, row_count, tile_rows, col_count, tile_cols)
    return returned.transpose(1, 3, 0, 2, 4)


def body(
    pair_state,
    residue_mask,
    input_gain,
    input_shift,
    left_right,
    output_gate,
    final_gain,
    final_shift,
    output_weight,
):
    tile_rows, tile_cols, channels = pair_state.shape
    hidden = output_weight.shape[0]
    normed_in = norm_over(pair_state.astype(jnp.float32), input_gain, input_shift, 2).astype(
        jnp.bfloat16
    )
    row_start = lax.axis_index("row") * tile_rows
    col_start = lax.axis_index(("col", "ksplit")) * tile_cols
    row_live = lax.dynamic_slice_in_dim(residue_mask, row_start, tile_rows).astype(jnp.float32)
    col_live = lax.dynamic_slice_in_dim(residue_mask, col_start, tile_cols).astype(jnp.float32)
    live_mask = row_live[:, None] * col_live[None, :]
    left_side = gated_side(normed_in, left_right[:, : 2 * hidden], live_mask, hidden)
    right_side = gated_side(normed_in, left_right[:, 2 * hidden :], live_mask, hidden)
    devices_all = lax.axis_size(("row", "col", "ksplit"))
    row_count = lax.axis_size("row")
    col_count = devices_all // row_count
    per_device = hidden // devices_all
    grouped_left = left_side.reshape(devices_all, per_device, tile_rows, tile_cols)
    grouped_right = right_side.reshape(devices_all, per_device, tile_rows, tile_cols)
    left_parts = lax.all_to_all(
        grouped_left, ("row", "col", "ksplit"), split_axis=0, concat_axis=0, tiled=True
    )
    right_parts = lax.all_to_all(
        grouped_right, ("row", "col", "ksplit"), split_axis=0, concat_axis=0, tiled=True
    )
    count_items = left_parts.shape[1]
    shaped_left = left_parts.reshape(row_count, col_count, count_items, tile_rows, tile_cols)
    shaped_right = right_parts.reshape(row_count, col_count, count_items, tile_rows, tile_cols)
    returned = contract_parts(shaped_left, shaped_right, row_count, col_count)
    returned = returned.reshape(devices_all, count_items, tile_rows, tile_cols)
    received = lax.all_to_all(
        returned, ("row", "col", "ksplit"), split_axis=0, concat_axis=0, tiled=True
    )
    mixed_tile = received.reshape(hidden, tile_rows, tile_cols)
    normed_out = norm_over(
        mixed_tile, final_gain[:, None, None], final_shift[:, None, None], 0
    ).astype(jnp.bfloat16)
    projected_out = jnp.einsum(
        "hij,hc->ijc", normed_out, output_weight, preferred_element_type=jnp.float32
    )
    gate_values = jax.nn.sigmoid(
        jnp.einsum("ijc,cd->ijd", normed_in, output_gate, preferred_element_type=jnp.float32)
    )
    return (gate_values * projected_out).astype(jnp.bfloat16)


def solution(mesh):
    placed = (
        P(("groups", "row"), ("col", "ksplit"), None),
        P("groups"),
        P(),
        P(),
        P(),
        P(),
        P(),
        P(),
        P(),
    )
    return jax.shard_map(
        update,
        mesh=mesh,
        in_specs=placed,
        out_specs=P(("groups", "row"), ("col", "ksplit"), None),
        check_vma=False,
    )
```
